32 devices in a mesh: gx: 2 (over y), gy: 4 (over x, core), gz: 4 (over z).
Axes of the slice: x: 2, y: 2, z: 4, core: 2. Of those that a mesh axis runs over, the one named last changes fastest.
Arguments:
- coordinates: float32 [2, 4, 4, 3, 16, 128], P('gx', 'gy', 'gz'), may hold values from -8 to 88
- neighbours: int32 [2, 4, 4, 16, 128], P('gx', 'gy', 'gz'), may hold values from 0 to 991, as said below
- pair_index: int32 [2, 4, 4, 4, 15360], P('gx', 'gy', 'gz'), may hold values from 0 to 127, as said below
- pair_live: int32 [2, 4, 4, 15360], P('gx', 'gy', 'gz'), may hold values 0 or 1
- basis: bfloat16 [2, 4, 4, 128, 1536], P('gx', 'gy', 'gz'), may hold values from -50 to 50
Outputs:
- next_basis: float32 [2, 4, 4, 128, 1536], P('gx', 'gy', 'gz')
- ritz_matrix: float32 [256, 256], replicated
The draws below stay inside these ranges and needn't reach their ends.
Inputs may be any that keep to these rules, and one draw needn't show every extreme that they name: neighbours[x, y, z, 0, f] = 864 + f. Any other entry c < 864 names frame c % 32 of the domain offset by (c // 32 // 9 - 1, c // 32 // 3 % 3 - 1, c // 32 % 3 - 1), which lies in the grid and is not the domain itself; an entry c >= 864 names the domain's own frame c - 864, never the row's frame f. `pair_index`: row 0 holds a frame f < 128, row 1 a slot 1 to 15, rows 2 and 3 atoms below 16.
All inputs are finite; a program needn't handle non-finite values. No bound on the sum of `pair_live` on one device may be relied on, other than what follows from the above.
Results may differ from the reference program's by a relative error of at most 0.0003.
Values may be sent and summed in bfloat16 or wider, within the bound.
No kernel may reach another device: no remote copies, remote signals or barrier semaphores. Data moves between devices by JAX's collectives and lax.ppermute only.
A program may use at most 128 MiB of HBM per device.

```python
import jax
import jax.numpy as jnp
from jax import lax

K = 256
F_DEV = 128
APF = 16
NBR = 16
BND = 32
PAIRS = 15360
GRID_X = 2
GRID_Y = 4
GRID_Z = 4
NROWS = 24576


def draw_coordinates(key, part):
    centre_key = jax.random.fold_in(key, 11)
    offset_key = jax.random.fold_in(key, 12)
    anchor = jnp.stack(jnp.meshgrid(jnp.arange(GRID_X), jnp.arange(GRID_Y), jnp.arange(GRID_Z), indexing='ij'), axis=3).astype(jnp.float32)
    centres = (anchor[:, :, :, :, None, None] + jax.random.uniform(centre_key, (GRID_X, GRID_Y, GRID_Z, 3, 1, F_DEV))) * 20.0
    offsets = 2.0 * jnp.clip(jax.random.normal(offset_key, (GRID_X, GRID_Y, GRID_Z, 3, APF, F_DEV)), -4.0, 4.0)
    return centres + offsets


def draw_neighbours(key, part):
    full_shape = (GRID_X, GRID_Y, GRID_Z, NBR, F_DEV)
    step_x = jax.random.randint(jax.random.fold_in(key, 21), full_shape, -1, 2)
    step_y = jax.random.randint(jax.random.fold_in(key, 22), full_shape, -1, 2)
    step_z = jax.random.randint(jax.random.fold_in(key, 23), full_shape, -1, 2)
    grid_x = jnp.arange(GRID_X, dtype=jnp.int32)[:, None, None, None, None]
    grid_y = jnp.arange(GRID_Y, dtype=jnp.int32)[None, :, None, None, None]
    grid_z = jnp.arange(GRID_Z, dtype=jnp.int32)[None, None, :, None, None]
    inside = (grid_x + step_x >= 0) & (grid_x + step_x < GRID_X)
    inside = inside & (grid_y + step_y >= 0) & (grid_y + step_y < GRID_Y)
    inside = inside & (grid_z + step_z >= 0) & (grid_z + step_z < GRID_Z)
    inside = inside & ((step_x != 0) | (step_y != 0) | (step_z != 0))
    ghost_frame = jax.random.randint(jax.random.fold_in(key, 24), full_shape, 0, BND)
    ghost_column = ((step_x + 1) * 9 + (step_y + 1) * 3 + (step_z + 1)) * BND + ghost_frame
    frame_ids = jnp.arange(F_DEV, dtype=jnp.int32)[None, None, None, None, :]
    other_frame = jax.random.randint(jax.random.fold_in(key, 25), full_shape, 1, F_DEV)
    local_column = 27 * BND + (frame_ids + other_frame) % F_DEV
    choose = jax.random.randint(jax.random.fold_in(key, 26), full_shape, 0, 2) == 0
    picked = jnp.where(choose & inside, ghost_column, local_column)
    slot_ids = jnp.arange(NBR, dtype=jnp.int32)[None, None, None, :, None]
    own_column = 27 * BND + frame_ids + jnp.zeros(full_shape, jnp.int32)
    return jnp.where(slot_ids == 0, own_column, picked).astype(jnp.int32)


def draw_pair_index(key, part):
    full_shape = (GRID_X, GRID_Y, GRID_Z, PAIRS)
    own_frame = jax.random.randint(jax.random.fold_in(key, 31), full_shape, 0, F_DEV)
    slot_of = jax.random.randint(jax.random.fold_in(key, 32), full_shape, 1, NBR)
    atom_a = jax.random.randint(jax.random.fold_in(key, 33), full_shape, 0, APF)
    atom_b = jax.random.randint(jax.random.fold_in(key, 34), full_shape, 0, APF)
    return jnp.stack([own_frame, slot_of, atom_a, atom_b], axis=3).astype(jnp.int32)


def draw_basis(key, part):
    scale_key = jax.random.fold_in(key, 41)
    value_key = jax.random.fold_in(key, 42)
    column_scale = jnp.exp(jax.random.uniform(scale_key, (GRID_X, GRID_Y, GRID_Z, 1, 6, K), minval=0.0, maxval=2.302585))
    values = column_scale * jnp.clip(jax.random.normal(value_key, (GRID_X, GRID_Y, GRID_Z, F_DEV, 6, K)), -4.0, 4.0)
    return values.reshape(GRID_X, GRID_Y, GRID_Z, F_DEV, 6 * K).astype(jnp.bfloat16)


def set_ends(entries, rng, smallest, largest):
    extent = entries.shape
    place = [jax.random.randint(jax.random.fold_in(rng, axis), (), 0, extent[axis]) for axis in range(len(extent))]
    entries = entries.at[tuple(place)].set(smallest)
    longest = extent.index(max(extent))
    place[longest] = (place[longest] + 1) % extent[longest]
    return entries.at[tuple(place)].set(largest)


def setup_inputs(seed: int = 0) -> dict:
    keys = jax.random.split(jax.random.key(seed), 6)
    return {
        "coordinates": draw_coordinates(jax.random.fold_in(keys[5], 71), 0),
        "neighbours": draw_neighbours(jax.random.fold_in(keys[5], 71), 0),
        "pair_index": draw_pair_index(jax.random.fold_in(keys[5], 71), 0),
        "pair_live": set_ends((jax.random.randint(keys[3], (GRID_X, GRID_Y, GRID_Z, PAIRS), 0, 4) < 3).astype(jnp.int32), jax.random.fold_in(keys[3], 1), 0, 1),
        "basis": draw_basis(jax.random.fold_in(keys[5], 71), 0),
    }


stiffness = 0.01

def cross_product(left, right):
    return jnp.stack([left[1] * right[2] - left[2] * right[1], left[2] * right[0] - left[0] * right[2], left[0] * right[1] - left[1] * right[0]])

def assemble(visible, neighbours, pair_index, pair_live):
    columns = visible.shape[2]
    frames = neighbours.shape[1]
    slots = neighbours.shape[0]
    centres = jnp.mean(visible, axis=1)
    own_frame = pair_index[0]
    slot_of = pair_index[1]
    atom_a = pair_index[2]
    atom_b = pair_index[3]
    self_column = own_frame + (columns - frames)
    partner = jnp.take(neighbours.reshape(-1), slot_of * frames + own_frame, axis=0)
    flat_coords = visible.reshape(3, -1)
    pos_a = jnp.take(flat_coords, atom_a * columns + self_column, axis=1)
    pos_b = jnp.take(flat_coords, atom_b * columns + partner, axis=1)
    arm_a = pos_a - jnp.take(centres, self_column, axis=1)
    arm_b = pos_b - jnp.take(centres, partner, axis=1)
    spring = pos_a - pos_b
    length_sq = jnp.maximum(jnp.sum(spring * spring, axis=0), 1.0)
    weight = stiffness * pair_live.astype(jnp.float32) / length_sq
    left_vec = jnp.concatenate([spring, cross_product(arm_a, spring)], axis=0)
    right_vec = jnp.concatenate([spring, cross_product(arm_b, spring)], axis=0)
    off_terms = -(weight * left_vec)[:, None, :] * right_vec[None, :, :]
    self_terms = (weight * left_vec)[:, None, :] * left_vec[None, :, :]
    values = jnp.concatenate([off_terms.reshape(36, -1).T, self_terms.reshape(36, -1).T], axis=0)
    row_keys = jnp.concatenate([slot_of * frames + own_frame, own_frame], axis=0).astype(jnp.int32)
    blocks = jnp.zeros((slots * frames, 36), jnp.float32).at[row_keys].add(values)
    return blocks.reshape(slots, frames, 36).transpose(0, 2, 1)

def apply_blocks(blocks, neighbours, vector_table):
    frames = neighbours.shape[1]
    vector_count = vector_table.shape[1] // 6

    def add_slot(slot_index, accumulated):
        gathered = jnp.take(vector_table, neighbours[slot_index], axis=0).reshape(frames, 6, vector_count)
        coeffs = blocks[slot_index].reshape(6, 6, frames)
        for inner_dof in range(6):
            accumulated = accumulated + coeffs[:, inner_dof, :].T[:, :, None] * gathered[:, None, inner_dof, :].astype(jnp.float32)
        return accumulated
    start = jnp.zeros((frames, 6, vector_count), jnp.float32)
    accumulated = lax.fori_loop(0, neighbours.shape[0], add_slot, start)
    return accumulated.reshape(frames, 6 * vector_count)

def gram_matrix(left, right):
    return lax.dot_general(left.astype(jnp.float32), right.astype(jnp.float32), (((0,), (0,)), ((), ())), preferred_element_type=jnp.float32)

def rayleigh_ritz(basis_gram, cross_gram, image_gram, image_rows, total_rows):
    factor = jnp.linalg.cholesky(basis_gram / total_rows)
    sym_cross = (cross_gram + cross_gram.T) / (2.0 * total_rows)
    half_solved = lax.linalg.triangular_solve(factor, sym_cross, left_side=True, lower=True)
    ritz_matrix = lax.linalg.triangular_solve(factor, half_solved.T, left_side=True, lower=True)
    image_factor = jnp.linalg.cholesky(image_gram / total_rows)
    next_rows = lax.linalg.triangular_solve(image_factor, image_rows, left_side=False, lower=True, transpose_a=True)
    return (ritz_matrix, next_rows)

def reference(coordinates, neighbours, pair_index, pair_live, basis):
    rim_coords = jnp.pad(coordinates[:, :, :, :, :, :BND], ((1, 1), (1, 1), (1, 1), (0, 0), (0, 0), (0, 0)))
    rim_basis = jnp.pad(basis[:, :, :, :BND, :], ((1, 1), (1, 1), (1, 1), (0, 0), (0, 0)))

    def one_domain(flat_index):
        dom_x = flat_index // (GRID_Y * GRID_Z)
        dom_y = flat_index // GRID_Z % GRID_Y
        dom_z = flat_index % GRID_Z
        zero_index = jnp.zeros((), jnp.int32)
        near_coords = lax.dynamic_slice(rim_coords, (dom_x, dom_y, dom_z, zero_index, zero_index, zero_index), (3, 3, 3, 3, APF, BND))
        near_basis = lax.dynamic_slice(rim_basis, (dom_x, dom_y, dom_z, zero_index, zero_index), (3, 3, 3, BND, 6 * K))
        own_coords = coordinates[dom_x, dom_y, dom_z]
        own_basis = basis[dom_x, dom_y, dom_z]
        own_lists = neighbours[dom_x, dom_y, dom_z]
        visible = jnp.concatenate([near_coords.reshape(27, 3, APF, BND).transpose(1, 2, 0, 3).reshape(3, APF, 27 * BND), own_coords], axis=2)
        vector_table = jnp.concatenate([near_basis.reshape(27 * BND, 6 * K), own_basis], axis=0)
        blocks = assemble(visible, own_lists, pair_index[dom_x, dom_y, dom_z], pair_live[dom_x, dom_y, dom_z])
        image_rows = apply_blocks(blocks, own_lists, vector_table)
        rounded = image_rows.astype(jnp.bfloat16).reshape(F_DEV * 6, K)
        flat_basis = own_basis.reshape(F_DEV * 6, K)
        grams = (gram_matrix(flat_basis, flat_basis), gram_matrix(flat_basis, rounded), gram_matrix(rounded, rounded))
        return (image_rows, grams)
    domain_ids = jnp.arange(GRID_X * GRID_Y * GRID_Z, dtype=jnp.int32)
    images, grams = lax.map(one_domain, domain_ids)
    basis_gram = jnp.sum(grams[0], axis=0)
    cross_gram = jnp.sum(grams[1], axis=0)
    image_gram = jnp.sum(grams[2], axis=0)
    ritz_matrix, next_rows = rayleigh_ritz(basis_gram, cross_gram, image_gram, images.reshape(-1, K), NROWS)
    next_basis = next_rows.reshape(GRID_X, GRID_Y, GRID_Z, F_DEV, 6 * K)
    return (next_basis, ritz_matrix)
```

```python
import functools

import jax
import jax.numpy as jnp
from jax import lax
from jax.experimental import pallas as pl
from jax.experimental.pallas import tpu as pltpu
from jax.sharding import PartitionSpec as P

stiffness = 0.01
radix = 4096.0
exact = lax.Precision.HIGHEST
f32 = jnp.float32
bf16 = jnp.bfloat16


def round_up(value, step):
    return (value + step - 1) // step * step


def count_kernel(index_ref, out_ref, *, frames, half, first, steps, chunk):
    rows, lanes = out_ref.shape[1:]
    row_ids = lax.broadcasted_iota(jnp.int32, (rows, chunk), 0).astype(jnp.int16)
    lane_ids = lax.broadcasted_iota(jnp.int32, (lanes, chunk), 0).astype(jnp.int16)
    zero = jnp.zeros((), bf16)
    out_ref[...] = jnp.zeros_like(out_ref)

    def one_chunk(i, carry):
        at = pl.ds(pl.multiple_of((first + i) * chunk, 128), chunk)
        block = index_ref[:, at]
        frame, slot, atom_a, atom_b, live = [block[k : k + 1] for k in range(5)]
        high = atom_b >= half
        row = (slot - 1) * (half * half) + jnp.where(high, atom_b - half, atom_b) * half
        high_a = atom_a >= half
        row = row + jnp.where(high_a, atom_a - half, atom_a)
        lane = jnp.where(high_a, frames, 0) + frame
        value = jnp.where(high, radix, 1.0) * live.astype(f32)
        left = jnp.where(row_ids == row.astype(jnp.int16), value.astype(bf16), zero)
        right = jnp.where(lane_ids == lane.astype(jnp.int16), jnp.ones((), bf16), zero)
        both = lax.dot_general(
            left, right, (((1,), (1,)), ((), ())), preferred_element_type=f32
        )
        upper = jnp.floor(both * (1.0 / radix))
        out_ref[0] += both - upper * radix
        out_ref[1] += upper
        return carry

    lax.fori_loop(0, steps, one_chunk, 0)


def count_pairs(pair_rows, frames, slots, atoms, first, steps, chunk):
    half = atoms // 2
    rows = (slots - 1) * half * half
    vmem = pl.BlockSpec(memory_space=pltpu.VMEM)
    return pl.pallas_call(
        functools.partial(
            count_kernel, frames=frames, half=half, first=first, steps=steps, chunk=chunk
        ),
        in_specs=[vmem],
        out_specs=vmem,
        out_shape=jax.ShapeDtypeStruct((2, rows, 2 * frames), f32),
        cost_estimate=pl.CostEstimate(
            flops=2 * rows * 2 * frames * chunk * steps,
            bytes_accessed=rows * frames * 16,
            transcendentals=0,
        ),
        name="count_pairs",
    )(pair_rows)


upper_pairs = [(i, j) for i in range(6) for j in range(i, 6)]
pair_slot = {}
for _n, (_i, _j) in enumerate(upper_pairs):
    pair_slot[(_i, _j)] = _n
    pair_slot[(_j, _i)] = _n


def split3(x):
    hi = x.astype(bf16)
    rest = x - hi.astype(f32)
    mid = rest.astype(bf16)
    low = (rest - mid.astype(f32)).astype(bf16)
    return hi, mid, low


def block_kernel(*refs, pieces, base):
    count_refs = refs[:2]
    piece_refs = refs[2 : 2 + pieces]
    own_ref, index_ref, out_ref, near_scr, sum_scr, arm_scr, blk_scr = refs[2 + pieces :]
    atoms, frames = own_ref.shape[1:]
    slots = index_ref.shape[0]
    half = atoms // 2
    width = 3 * atoms
    near_scr[...] = jnp.zeros_like(near_scr)
    start = 0
    for piece in piece_refs:
        for k in range(piece.shape[0]):
            near_scr[start : start + piece.shape[1], 0:width] = piece[k]
            start += piece.shape[1]
    near = near_scr[...].T[0:width]
    own = own_ref[...].reshape(width, frames)
    parts = [jnp.concatenate([n, o], axis=1) for n, o in zip(split3(near), split3(own))]
    left = jnp.concatenate(parts, axis=0)
    rows = base + frames
    row_ids = lax.broadcasted_iota(jnp.int32, (rows, frames), 0)
    pos = [own_ref[c] for c in range(3)]
    centre = [jnp.mean(p, axis=0, keepdims=True) for p in pos]
    pos_t = [[p[h * half : (h + 1) * half] for h in range(2)] for p in pos]
    rho_t = [[p - c for p in pt] for pt, c in zip(pos_t, centre)]
    sum_scr[...] = jnp.zeros_like(sum_scr)
    arm_scr[...] = jnp.zeros_like(arm_scr)

    def one_slot(s, carry):
        pick = index_ref[pl.ds(s, 1), :]
        hot = jnp.where(row_ids == pick, 1.0, 0.0).astype(bf16)
        got = jnp.dot(left, hot, preferred_element_type=f32)
        far = got[0:width] + got[width : 2 * width] + got[2 * width : 3 * width]
        far = [far[c * atoms : (c + 1) * atoms] for c in range(3)]
        for c in range(3):
            arm_scr[c, pl.ds(s, 1), :] = jnp.mean(far[c], axis=0, keepdims=True) - centre[c]
        moments = [[None] * 6 for _ in range(2)]
        for b in range(atoms):
            at = pl.multiple_of((s - 1) * (half * half) + (b % half) * half, half)
            q = [jnp.broadcast_to(far[c][b : b + 1, :], (half, frames)) for c in range(3)]
            for h in range(2):
                lanes = slice(h * frames, (h + 1) * frames)
                n = count_refs[0][b // half, pl.ds(at, half), lanes]
                n = n + count_refs[1][b // half, pl.ds(at, half), lanes]
                d = [pos_t[c][h] - q[c] for c in range(3)]
                w = n / jnp.maximum(d[0] * d[0] + d[1] * d[1] + d[2] * d[2], 1.0)
                wd = [w * d[c] for c in range(3)]
                terms = [wd[0] * d[0], wd[0] * d[1], wd[0] * d[2], wd[1] * d[1], wd[1] * d[2], wd[2] * d[2]]
                m = moments[h]
                moments[h] = terms if m[0] is None else [x + y for x, y in zip(m, terms)]
        total = [None] * 21
        for h in range(2):
            m = moments[h]
            r = [rho_t[c][h] for c in range(3)]
            dd = [[m[0], m[1], m[2]], [m[1], m[3], m[4]], [m[2], m[4], m[5]]]
            dt = [
                [
                    r[1] * dd[i][2] - r[2] * dd[i][1],
                    r[2] * dd[i][0] - r[0] * dd[i][2],
                    r[0] * dd[i][1] - r[1] * dd[i][0],
                ]
                for i in range(3)
            ]
            tt = {}
            for j in range(3):
                col = [dt[0][j], dt[1][j], dt[2][j]]
                tt[(0, j)] = r[1] * col[2] - r[2] * col[1]
                tt[(1, j)] = r[2] * col[0] - r[0] * col[2]
                tt[(2, j)] = r[0] * col[1] - r[1] * col[0]
            for n, (i, j) in enumerate(upper_pairs):
                if j < 3:
                    x = dd[i][j]
                elif i < 3:
                    x = dt[i][j - 3]
                else:
                    x = tt[(i - 3, j - 3)]
                total[n] = x if total[n] is None else total[n] + x
        for n in range(21):
            sum_scr[n, pl.ds(s, 1), :] = jnp.sum(total[n], axis=0, keepdims=True) * stiffness
        return carry

    lax.fori_loop(1, slots, one_slot, 0)
    first = lax.broadcasted_iota(jnp.int32, (slots, frames), 0) == 0
    arm = [arm_scr[c] for c in range(3)]
    sums = [sum_scr[n] for n in range(21)]
    selfs = [jnp.sum(x, axis=0, keepdims=True) for x in sums]
    blk_scr[...] = jnp.zeros_like(blk_scr)
    out_ref[...] = jnp.zeros_like(out_ref)
    for j in range(6):
        for i in range(6):
            x = sums[pair_slot[(j, i)]]
            if i >= 3:
                p, q = (i - 2) % 3, (i - 1) % 3
                x = x - (arm[p] * sums[pair_slot[(j, q)]] - arm[q] * sums[pair_slot[(j, p)]])
            x = jnp.where(first, selfs[pair_slot[(j, i)]], -x)
            for h in range(2):
                blk_scr[j, pl.ds(2 * i + h, slots, stride=16), :] = x
        turned = blk_scr[j, 0 : slots * 16, :].T
        for h in range(turned.shape[1] // 128):
            out_ref[h, pl.ds(j, frames, stride=8), :] = turned[:, h * 128 : (h + 1) * 128]


def make_blocks(counts, pieces, own, index, base):
    slots, frames = index.shape
    vmem = pl.BlockSpec(memory_space=pltpu.VMEM)
    return pl.pallas_call(
        functools.partial(block_kernel, pieces=len(pieces), base=base),
        in_specs=[vmem] * (4 + len(pieces)),
        out_specs=vmem,
        out_shape=jax.ShapeDtypeStruct((slots // 8, frames * 8 + 8, 128), f32),
        scratch_shapes=[
            pltpu.VMEM((base, 128), f32),
            pltpu.VMEM((21, slots, frames), f32),
            pltpu.VMEM((3, slots, frames), f32),
            pltpu.VMEM((6, slots * 16 + 16, frames), f32),
        ],
        cost_estimate=pl.CostEstimate(flops=10**9, bytes_accessed=8 * 10**6, transcendentals=0),
        name="make_blocks",
    )(*counts, *pieces, own, index)


def apply_kernel(*refs, pieces, base):
    index_ref, coeff_ref = refs[:2]
    piece_refs = refs[2 : 2 + pieces]
    own_ref, image_ref, gram_ref, tab_scr, own_scr = refs[2 + pieces :]
    frames = own_ref.shape[0]
    slots = index_ref.shape[0]
    vectors = own_ref.shape[1] // 6
    tiles = own_ref.shape[1] // 128
    rim = piece_refs[0].shape[1]
    start = 0
    for piece in piece_refs:

        def fill(k, carry, piece=piece, start=start):
            at = (start + k) * (rim * 16)
            for t in range(tiles):
                part = piece[k, :, t * 128 : (t + 1) * 128].astype(f32)
                tab_scr[pl.ds(at + t, rim, stride=16), :] = part
            for t in range(tiles, 16):
                tab_scr[pl.ds(at + t, rim, stride=16), :] = jnp.zeros((rim, 128), f32)
            return carry

        lax.fori_loop(0, piece.shape[0], fill, 0)
        start += piece.shape[0]
    for t in range(16):
        if t < tiles:
            part = own_ref[:, t * 128 : (t + 1) * 128].astype(f32)
        else:
            part = jnp.zeros((frames, 128), f32)
        tab_scr[pl.ds(base * 16 + t, frames, stride=16), :] = part
    for h in range(2):
        for j in range(8):
            if j < 6:
                at = j * vectors + h * 128
                part = own_ref[:, at : at + 128].astype(f32)
            else:
                part = jnp.zeros((frames, 128), f32)
            own_scr[h, pl.ds(j, frames, stride=8), :] = part
    odd = lax.broadcasted_iota(jnp.int32, (8, slots * 16), 1) % 2 == 1

    def one_frame(f, carry):
        got = []
        for s in range(slots):
            at = pl.multiple_of(index_ref[s, f] * 16, 16)
            got.append(tab_scr[pl.ds(at, 16), :].astype(bf16))
        right = jnp.concatenate(got, axis=0)
        at = pl.multiple_of(f * 8, 8)
        coeff = jnp.concatenate([coeff_ref[h, pl.ds(at, 8), :] for h in range(slots // 8)], axis=1)
        wide = jnp.concatenate([jnp.where(odd, 0.0, coeff), jnp.where(odd, coeff, 0.0)], axis=0)
        high = wide.astype(bf16)
        low = (wide - high.astype(f32)).astype(bf16)
        res = jnp.dot(jnp.concatenate([high, low], axis=0), right, preferred_element_type=f32)
        res = res[0:16] + res[16:32]
        image_ref[pl.ds(at, 8), 0:128] = res[0:8]
        image_ref[pl.ds(at, 8), 128:256] = res[8:16]
        return carry

    lax.fori_loop(0, frames, one_frame, 0, unroll=4)
    dims = (((0,), (0,)), ((), ()))
    x = jnp.concatenate([own_scr[h, 0 : frames * 8, :] for h in range(2)], axis=1).astype(bf16)
    y = image_ref[...].astype(bf16)
    basis_gram = lax.dot_general(x, x, dims, preferred_element_type=f32)
    cross = lax.dot_general(x, y, dims, preferred_element_type=f32)
    image_gram = lax.dot_general(y, y, dims, preferred_element_type=f32)
    cross = cross + cross.T
    rows = lax.broadcasted_iota(jnp.int32, cross.shape, 0)
    cols = lax.broadcasted_iota(jnp.int32, cross.shape, 1)
    last = vectors - 1
    corner = jnp.sum(jnp.where((rows == last) & (cols == last), cross, 0.0), axis=0, keepdims=True)
    diag = jnp.where((rows == cols) & (rows < last), cross, 0.0)
    diag = pltpu.roll(diag, 1, 1) + jnp.where(rows == 0, corner, 0.0)
    gram_ref[0] = jnp.where(rows >= cols, image_gram, cross)
    gram_ref[1] = jnp.where(rows >= cols, basis_gram, diag)


def apply_blocks(index, coeff, pieces, own, base):
    slots, frames = index.shape
    vectors = own.shape[1] // 6
    vmem = pl.BlockSpec(memory_space=pltpu.VMEM)
    return pl.pallas_call(
        functools.partial(apply_kernel, pieces=len(pieces), base=base),
        in_specs=[pl.BlockSpec(memory_space=pltpu.SMEM)] + [vmem] * (2 + len(pieces)),
        out_specs=(vmem, vmem),
        out_shape=(
            jax.ShapeDtypeStruct((frames * 8, vectors), f32),
            jax.ShapeDtypeStruct((2, vectors, vectors), f32),
        ),
        scratch_shapes=[
            pltpu.VMEM(((base + frames) * 16 + 16, 128), f32),
            pltpu.VMEM((2, frames * 8 + 8, 128), f32),
        ],
        cost_estimate=pl.CostEstimate(flops=10**9, bytes_accessed=8 * 10**6, transcendentals=0),
        name="apply_blocks",
    )(index, coeff, *pieces, own)


panel = 64


def factor_panel(block):
    groups = panel // 8
    sub = lax.broadcasted_iota(jnp.int32, (8, 128), 0)
    rows = [block[g * 8 : (g + 1) * 8] for g in range(groups)]
    for g in range(groups):
        wide = [
            [jnp.broadcast_to(rows[r][:, g * 8 + k : g * 8 + k + 1], (8, 128)) for k in range(8)]
            for r in range(g, groups)
        ]
        lead = wide[0]
        top = rows[g]
        inverse = []
        scale = jnp.zeros((8, 128), f32)
        for k in range(8):
            pivot = jnp.broadcast_to(lead[k][k : k + 1, :], (8, 128))
            inv = 1.0 / pivot
            inverse.append(inv)
            scale = jnp.where(sub == k, lax.rsqrt(pivot), scale)
            factor = jnp.where(sub > k, lead[k] * inv, 0.0)
            top_row = jnp.broadcast_to(top[k : k + 1, :], (8, 128))
            top = top - factor * top_row
            for m in range(k + 1, 8):
                lead[m] = lead[m] - factor * jnp.broadcast_to(lead[m][k : k + 1, :], (8, 128))
        for r in range(g + 1, groups):
            cols = wide[r - g]
            row = rows[r]
            for k in range(8):
                factor = cols[k] * inverse[k]
                row = row - factor * jnp.broadcast_to(top[k : k + 1, :], (8, 128))
                for m in range(k + 1, 8):
                    cols[m] = cols[m] - factor * jnp.broadcast_to(lead[m][k : k + 1, :], (8, 128))
            rows[r] = row
        rows[g] = top * scale
    return jnp.concatenate(rows, axis=0)


def solve_kernel(gram_ref, image_ref, next_ref, ritz_ref, mat_scr, res_scr, *, total_rows):
    size = gram_ref.shape[1]
    frames = next_ref.shape[0]
    rows = lax.broadcasted_iota(jnp.int32, (size, size), 0)
    cols = lax.broadcasted_iota(jnp.int32, (size, size), 1)
    mixed = gram_ref[0] * (1.0 / total_rows)
    other = gram_ref[1] * (1.0 / total_rows)
    turned = mixed.T
    image_gram = jnp.where(rows >= cols, mixed, turned)
    basis_gram = jnp.where(rows >= cols, other, other.T)
    last = size - 1
    diag = pltpu.roll(jnp.where(cols == rows + 1, other, 0.0), size - 1, 1)
    corner = jnp.sum(jnp.where((rows == 0) & (cols == last), other, 0.0), axis=0, keepdims=True)
    diag = diag + jnp.where(rows == last, corner, 0.0)
    cross = jnp.where(rows < cols, mixed, jnp.where(rows > cols, turned, diag)) * 0.5
    eye = jnp.where(rows == cols, 1.0, 0.0)
    mat_scr[0, :, 0:size] = image_gram
    mat_scr[1, :, 0:size] = basis_gram
    mat_scr[0, :, size:] = eye
    mat_scr[1, :, size:] = eye
    small = jnp.where(
        lax.broadcasted_iota(jnp.int32, (panel, panel), 0)
        == lax.broadcasted_iota(jnp.int32, (panel, panel), 1),
        1.0,
        0.0,
    )
    lane_ids = lax.broadcasted_iota(jnp.int32, (panel, size), 1)
    for p in range(size // panel):
        at = p * panel
        for m in range(2):
            strip = mat_scr[m, at : at + panel, :]
            block = jnp.concatenate([strip[:, at : at + panel], small], axis=1)
            inv = factor_panel(block)[:, panel:]
            done = jnp.dot(inv, strip, precision=exact, preferred_element_type=f32)
            mat_scr[m, at : at + panel, :] = done
            if at + panel < size:
                left = jnp.where(lane_ids >= at + panel, done[:, 0:size], 0.0)
                mat_scr[m] = mat_scr[m] - lax.dot_general(
                    left, done, (((0,), (0,)), ((), ())), precision=exact, preferred_element_type=f32
                )
    image_inv = mat_scr[0, :, size:]
    basis_inv = mat_scr[1, :, size:]
    turn = (((1,), (1,)), ((), ()))
    res = lax.dot_general(image_ref[...], image_inv, turn, precision=exact, preferred_element_type=f32)
    for h in range(size // 128):
        res_scr[h, 0 : frames * 8, :] = res[:, h * 128 : (h + 1) * 128]
    for j in range(6):
        for h in range(size // 128):
            at = j * size + h * 128
            next_ref[:, at : at + 128] = res_scr[h, pl.ds(j, frames, stride=8), :]
    half = jnp.dot(basis_inv, cross, precision=exact, preferred_element_type=f32)
    ritz_ref[...] = lax.dot_general(half, basis_inv, turn, precision=exact, preferred_element_type=f32)


def solve(gram, image, total_rows):
    size = image.shape[1]
    frames = image.shape[0] // 8
    vmem = pl.BlockSpec(memory_space=pltpu.VMEM)
    return pl.pallas_call(
        functools.partial(solve_kernel, total_rows=float(total_rows)),
        in_specs=[vmem, vmem],
        out_specs=(vmem, vmem),
        out_shape=(
            jax.ShapeDtypeStruct((frames, 6 * size), f32),
            jax.ShapeDtypeStruct((size, size), f32),
        ),
        scratch_shapes=[
            pltpu.VMEM((2, size, 2 * size), f32),
            pltpu.VMEM((size // 128, frames * 8 + 8, 128), f32),
        ],
        cost_estimate=pl.CostEstimate(flops=10**9, bytes_accessed=3 * 10**6, transcendentals=0),
        name="solve",
    )(gram, image)


def spread(stack, axis):
    count = lax.axis_size(axis)
    if count == 1:
        return [stack]
    up = [(i, i + 1) for i in range(count - 1)]
    down = [(i + 1, i) for i in range(count - 1)]
    if count == 2:
        return [stack, lax.ppermute(stack, axis, up + down)]
    return [stack, lax.ppermute(stack, axis, up), lax.ppermute(stack, axis, down)]


def place_of(offset, axis):
    count = lax.axis_size(axis)
    if count <= 2:
        return jnp.where(offset == 1, 0, 1), count
    return jnp.where(offset == 1, 0, jnp.where(offset == 0, 1, 2)), 3


def collect(rim):
    first = spread(rim, "gx")
    second = spread(jnp.concatenate(first, axis=0), "gz")
    return spread(jnp.concatenate(second, axis=0), "gy")


def sum_all(values, axes, halvings):
    steps = []
    for axis in axes:
        bit = 1
        while bit < lax.axis_size(axis):
            steps.append((axis, bit))
            bit *= 2
    trail = []
    for n, (axis, bit) in enumerate(steps):
        pairs = [(i, i ^ bit) for i in range(lax.axis_size(axis))]
        if n >= halvings:
            values = values + lax.ppermute(values, axis, pairs)
            continue
        high = (lax.axis_index(axis) & bit) != 0
        half = values.shape[0] // 2
        front, back = values[:half], values[half:]
        got = lax.ppermute(jnp.where(high, front, back), axis, pairs)
        values = jnp.where(high, back, front) + got
        trail.append((axis, high, pairs))
    for axis, high, pairs in reversed(trail):
        got = lax.ppermute(values, axis, pairs)
        values = jnp.where(
            high, jnp.concatenate([got, values]), jnp.concatenate([values, got])
        )
    return values


def per_device(coordinates, neighbours, pair_index, pair_live, basis):
    frames, columns = basis.shape[3:]
    rim = frames // 4
    atoms = coordinates.shape[4]
    slots = neighbours.shape[3]
    pairs = pair_index.shape[4]
    axes = ("gx", "gy", "gz")
    total_rows = 6 * frames
    for a in axes:
        total_rows *= lax.axis_size(a)
    own_coords = coordinates[0, 0, 0]
    own_basis = basis[0, 0, 0]
    lists = neighbours[0, 0, 0]

    rim_coords = own_coords.reshape(3 * atoms, frames)[:, :rim].T[None]
    near_coords = collect(rim_coords)
    near_basis = collect(own_basis[None, :rim])

    ghost = 27 * rim
    domain = lists // rim
    px, nx = place_of(domain // 9, "gx")
    py, ny = place_of(domain // 3 % 3, "gy")
    pz, nz = place_of(domain % 3, "gz")
    base = round_up(nx * ny * nz * rim, 128)
    index = jnp.where(
        lists < ghost,
        ((py * nz + pz) * nx + px) * rim + lists % rim,
        lists - ghost + base,
    )

    chunk = 1920
    steps = pairs // chunk
    cut = steps // 2
    pair_rows = jnp.concatenate(
        [pair_index[0, 0, 0], pair_live[0, 0], jnp.zeros((3, pairs), jnp.int32)], axis=0
    )
    counts = [
        count_pairs(pair_rows, frames, slots, atoms, 0, cut, chunk),
        count_pairs(pair_rows, frames, slots, atoms, cut, steps - cut, chunk),
    ]
    coeff = make_blocks(counts, near_coords, own_coords, index, base)
    image, gram = apply_blocks(index, coeff, near_basis, own_basis, base)
    size = gram.shape[1]
    gram = sum_all(gram.reshape(2 * size, size), ("gy", "gz", "gx"), 2).reshape(2, size, size)
    next_rows, ritz = solve(gram, image, total_rows)
    return next_rows[None, None, None], ritz


def solution(mesh):
    placed = (
        P("gx", "gy", "gz", None, None, None),
        P("gx", "gy", "gz", None, None),
        P("gx", "gy", "gz", None, None),
        P("gx", "gy", "gz", None),
        P("gx", "gy", "gz", None, None),
    )
    return jax.shard_map(
        per_device,
        mesh=mesh,
        in_specs=placed,
        out_specs=(P("gx", "gy", "gz", None, None), P()),
        check_vma=False,
    )
```

```python
import functools

import jax
import jax.numpy as jnp
from jax import lax
from jax.experimental import pallas as pl
from jax.experimental.pallas import tpu as pltpu
from jax.sharding import PartitionSpec as P

stiffness = 0.01
radix = 4096.0
exact = lax.Precision.HIGHEST
f32 = jnp.float32
bf16 = jnp.bfloat16


def near_core(x):
    return pltpu.with_memory_space_constraint(x, pltpu.VMEM)


def round_up(value, step):
    return (value + step - 1) // step * step


def count_kernel(*refs, frames, half, first, steps, chunk):
    index_ref, *before, out_ref = refs
    rows, lanes = out_ref.shape[1:]
    row_ids = lax.broadcasted_iota(jnp.int32, (rows, chunk), 0).astype(jnp.int16)
    lane_ids = lax.broadcasted_iota(jnp.int32, (lanes, chunk), 0).astype(jnp.int16)
    zero = jnp.zeros((), bf16)
    out_ref[...] = before[0][...] if before else jnp.zeros_like(out_ref)

    def one_chunk(i, carry):
        at = pl.ds(pl.multiple_of((first + i) * chunk, 128), chunk)
        block = index_ref[:, at]
        frame, slot, atom_a, atom_b, live = [block[k : k + 1] for k in range(5)]
        high = atom_b >= half
        row = (slot - 1) * (half * half) + jnp.where(high, atom_b - half, atom_b) * half
        high_a = atom_a >= half
        row = row + jnp.where(high_a, atom_a - half, atom_a)
        lane = jnp.where(high_a, frames, 0) + frame
        value = jnp.where(high, radix, 1.0) * live.astype(f32)
        left = jnp.where(row_ids == row.astype(jnp.int16), value.astype(bf16), zero)
        right = jnp.where(lane_ids == lane.astype(jnp.int16), jnp.ones((), bf16), zero)
        both = lax.dot_general(
            left, right, (((1,), (1,)), ((), ())), preferred_element_type=f32
        )
        upper = jnp.floor(both * (1.0 / radix))
        out_ref[0] += both - upper * radix
        out_ref[1] += upper
        return carry

    lax.fori_loop(0, steps, one_chunk, 0)


def count_pairs(before, table, frames, slots, atoms, first, steps, chunk):
    half = atoms // 2
    rows = (slots - 1) * half * half
    vmem = pl.BlockSpec(memory_space=pltpu.VMEM)
    return pl.pallas_call(
        functools.partial(
            count_kernel, frames=frames, half=half, first=first, steps=steps, chunk=chunk
        ),
        in_specs=[vmem] * (1 + len(before)),
        out_specs=vmem,
        out_shape=pltpu.VMEM((2, rows, 2 * frames), f32),
        cost_estimate=pl.CostEstimate(
            flops=2 * rows * 2 * frames * chunk * steps,
            bytes_accessed=rows * frames * 16,
            transcendentals=0,
        ),
        compiler_params=pltpu.CompilerParams(vmem_limit_bytes=24 << 20),
        name="count_pairs",
    )(near_core(table), *map(near_core, before))


upper_pairs = [(i, j) for i in range(6) for j in range(i, 6)]
pair_slot = {}
for _n, (_i, _j) in enumerate(upper_pairs):
    pair_slot[(_i, _j)] = _n
    pair_slot[(_j, _i)] = _n


def split3(x):
    hi = x.astype(bf16)
    rest = x - hi.astype(f32)
    mid = rest.astype(bf16)
    low = (rest - mid.astype(f32)).astype(bf16)
    return hi, mid, low


def block_kernel(*refs, pieces, base, columns):
    count_ref = refs[0]
    piece_refs = refs[1 : 1 + pieces]
    own_ref, index_ref, out_ref, near_scr, sum_scr, arm_scr, blk_scr = refs[1 + pieces :]
    atoms, frames = own_ref.shape[1:]
    slots = index_ref.shape[0]
    half = atoms // 2
    width = 3 * atoms
    near_scr[...] = jnp.zeros_like(near_scr)
    start = 0
    for piece in piece_refs:
        for k in range(piece.shape[0]):
            near_scr[start : start + piece.shape[1], :] = piece[k, :, columns:].astype(f32)
            start += piece.shape[1]
    near = near_scr[...].T[0 : 3 * width].astype(bf16)
    near = [near[k * width : (k + 1) * width] for k in range(3)]
    own = own_ref[...].reshape(width, frames)
    parts = [jnp.concatenate([n, o], axis=1) for n, o in zip(near, split3(own))]
    left = jnp.concatenate(parts, axis=0)
    rows = base + frames
    row_ids = lax.broadcasted_iota(jnp.int32, (rows, frames), 0)
    pos = [own_ref[c] for c in range(3)]
    centre = [jnp.mean(p, axis=0, keepdims=True) for p in pos]
    pos_t = [[p[h * half : (h + 1) * half] for h in range(2)] for p in pos]
    rho_t = [[p - c for p in pt] for pt, c in zip(pos_t, centre)]
    sum_scr[...] = jnp.zeros_like(sum_scr)
    arm_scr[...] = jnp.zeros_like(arm_scr)

    def one_slot(s, carry):
        pick = index_ref[pl.ds(s, 1), :]
        hot = jnp.where(row_ids == pick, 1.0, 0.0).astype(bf16)
        got = jnp.dot(left, hot, preferred_element_type=f32)
        far = got[0:width] + got[width : 2 * width] + got[2 * width : 3 * width]
        far = [far[c * atoms : (c + 1) * atoms] for c in range(3)]
        for c in range(3):
            arm_scr[c, pl.ds(s, 1), :] = jnp.mean(far[c], axis=0, keepdims=True) - centre[c]
        moments = [[None] * 6 for _ in range(2)]
        for b in range(atoms):
            at = pl.multiple_of((s - 1) * (half * half) + (b % half) * half, half)
            q = [jnp.broadcast_to(far[c][b : b + 1, :], (half, frames)) for c in range(3)]
            for h in range(2):
                lanes = slice(h * frames, (h + 1) * frames)
                n = count_ref[b // half, pl.ds(at, half), lanes]
                d = [pos_t[c][h] - q[c] for c in range(3)]
                w = n / jnp.maximum(d[0] * d[0] + d[1] * d[1] + d[2] * d[2], 1.0)
                wd = [w * d[c] for c in range(3)]
                terms = [wd[0] * d[0], wd[0] * d[1], wd[0] * d[2], wd[1] * d[1], wd[1] * d[2], wd[2] * d[2]]
                m = moments[h]
                moments[h] = terms if m[0] is None else [x + y for x, y in zip(m, terms)]
        total = [None] * 21
        for h in range(2):
            m = moments[h]
            r = [rho_t[c][h] for c in range(3)]
            dd = [[m[0], m[1], m[2]], [m[1], m[3], m[4]], [m[2], m[4], m[5]]]
            dt = [
                [
                    r[1] * dd[i][2] - r[2] * dd[i][1],
                    r[2] * dd[i][0] - r[0] * dd[i][2],
                    r[0] * dd[i][1] - r[1] * dd[i][0],
                ]
                for i in range(3)
            ]
            tt = {}
            for j in range(3):
                col = [dt[0][j], dt[1][j], dt[2][j]]
                tt[(0, j)] = r[1] * col[2] - r[2] * col[1]
                tt[(1, j)] = r[2] * col[0] - r[0] * col[2]
                tt[(2, j)] = r[0] * col[1] - r[1] * col[0]
            for n, (i, j) in enumerate(upper_pairs):
                if j < 3:
                    x = dd[i][j]
                elif i < 3:
                    x = dt[i][j - 3]
                else:
                    x = tt[(i - 3, j - 3)]
                total[n] = x if total[n] is None else total[n] + x
        for n in range(21):
            sum_scr[n, pl.ds(s, 1), :] = jnp.sum(total[n], axis=0, keepdims=True) * stiffness
        return carry

    lax.fori_loop(1, slots, one_slot, 0)
    first = lax.broadcasted_iota(jnp.int32, (slots, frames), 0) == 0
    arm = [arm_scr[c] for c in range(3)]
    sums = [sum_scr[n] for n in range(21)]
    selfs = [jnp.sum(x, axis=0, keepdims=True) for x in sums]
    blk_scr[...] = jnp.zeros_like(blk_scr)
    out_ref[...] = jnp.zeros_like(out_ref)
    for j in range(6):
        for i in range(6):
            x = sums[pair_slot[(j, i)]]
            if i >= 3:
                p, q = (i - 2) % 3, (i - 1) % 3
                x = x - (arm[p] * sums[pair_slot[(j, q)]] - arm[q] * sums[pair_slot[(j, p)]])
            x = jnp.where(first, selfs[pair_slot[(j, i)]], -x)
            for h in range(2):
                blk_scr[j, pl.ds(2 * i + h, slots, stride=17), :] = x
        turned = jnp.concatenate([blk_scr[j, s * 17 : s * 17 + 16, :] for s in range(slots)], axis=0).T
        for h in range(turned.shape[1] // 128):
            out_ref[h, pl.ds(j, frames, stride=9), :] = turned[:, h * 128 : (h + 1) * 128]


def make_blocks(counts, pieces, own, index, base, columns):
    slots, frames = index.shape
    vmem = pl.BlockSpec(memory_space=pltpu.VMEM)
    return pl.pallas_call(
        functools.partial(block_kernel, pieces=len(pieces), base=base, columns=columns),
        in_specs=[vmem] * (3 + len(pieces)),
        out_specs=vmem,
        out_shape=pltpu.VMEM((slots // 8, frames * 9 + 16, 128), f32),
        scratch_shapes=[
            pltpu.VMEM((base, pieces[0].shape[2] - columns), f32),
            pltpu.VMEM((21, slots, frames), f32),
            pltpu.VMEM((3, slots, frames), f32),
            pltpu.VMEM((6, slots * 17 + 17, frames), f32),
        ],
        cost_estimate=pl.CostEstimate(flops=10**9, bytes_accessed=8 * 10**6, transcendentals=0),
        compiler_params=pltpu.CompilerParams(vmem_limit_bytes=20 << 20),
        name="make_blocks",
    )(near_core(counts), *map(near_core, pieces), own, index)


def apply_kernel(*refs, pieces, base):
    index_ref, high_ref, coeff_ref = refs[:3]
    piece_refs = refs[3 : 3 + pieces]
    own_ref, image_ref, keep_ref, send_ref, tab_scr, image_scr = refs[3 + pieces :]
    frames = own_ref.shape[0]
    slots = index_ref.shape[0]
    vectors = own_ref.shape[1] // 6
    tiles = own_ref.shape[1] // 128
    pitch = tiles + 1
    rim = piece_refs[0].shape[1]
    start = 0
    for piece in piece_refs:

        def fill(k, carry, piece=piece, start=start):
            at = (start + k) * (rim * pitch)
            for t in range(tiles):
                part = piece[k, :, t * 128 : (t + 1) * 128].astype(f32)
                tab_scr[pl.ds(at + t, rim, stride=pitch), :] = part
            tab_scr[pl.ds(at + tiles, rim, stride=pitch), :] = jnp.zeros((rim, 128), f32)
            return carry

        lax.fori_loop(0, piece.shape[0], fill, 0)
        start += piece.shape[0]
    for t in range(tiles):
        part = own_ref[:, t * 128 : (t + 1) * 128].astype(f32)
        tab_scr[pl.ds(base * pitch + t, frames, stride=pitch), :] = part
    tab_scr[pl.ds(base * pitch + tiles, frames, stride=pitch), :] = jnp.zeros((frames, 128), f32)
    tab_scr[(base + frames) * pitch :, :] = jnp.zeros((16, 128), f32)
    odd = lax.broadcasted_iota(jnp.int32, (8, slots * 16), 1) % 2 == 1

    def one_frame(f, carry):
        got = []
        for s in range(slots):
            got.append(tab_scr[pl.ds(index_ref[s, f] * pitch, 16), :].astype(bf16))
        right = jnp.concatenate(got, axis=0)
        at = f * 9
        coeff = jnp.concatenate([coeff_ref[h, pl.ds(at, 8), :] for h in range(slots // 8)], axis=1)
        wide = jnp.concatenate([jnp.where(odd, 0.0, coeff), jnp.where(odd, coeff, 0.0)], axis=0)
        high = wide.astype(bf16)
        low = (wide - high.astype(f32)).astype(bf16)
        res = jnp.dot(jnp.concatenate([high, low], axis=0), right, preferred_element_type=f32)
        res = res[0:16] + res[16:32]
        image_scr[0, pl.ds(at, 8), :] = res[0:8]
        image_scr[1, pl.ds(at, 8), :] = res[8:16]
        return carry

    lax.fori_loop(0, frames, one_frame, 0, unroll=4)
    dims = (((0,), (0,)), ((), ()))
    basis_gram = jnp.zeros((vectors, vectors), f32)
    cross = jnp.zeros((vectors, vectors), f32)
    image_gram = jnp.zeros((vectors, vectors), f32)
    for j in range(6):
        x = own_ref[:, j * vectors : (j + 1) * vectors]
        y = jnp.concatenate([image_scr[h, pl.ds(j, frames, stride=9), :] for h in range(2)], axis=1)
        image_ref[j * frames : (j + 1) * frames, :] = y
        y = y.astype(bf16)
        basis_gram = basis_gram + lax.dot_general(x, x, dims, preferred_element_type=f32)
        cross = cross + lax.dot_general(x, y, dims, preferred_element_type=f32)
        image_gram = image_gram + lax.dot_general(y, y, dims, preferred_element_type=f32)
    cross = cross + cross.T
    rows = lax.broadcasted_iota(jnp.int32, cross.shape, 0)
    cols = lax.broadcasted_iota(jnp.int32, cross.shape, 1)
    last = vectors - 1
    corner = jnp.sum(jnp.where((rows == last) & (cols == last), cross, 0.0), axis=0, keepdims=True)
    diag = jnp.where((rows == cols) & (rows < last), cross, 0.0)
    diag = pltpu.roll(diag, 1, 1) + jnp.where(rows == 0, corner, 0.0)
    front = jnp.where(rows >= cols, image_gram, cross)
    back = jnp.where(rows >= cols, basis_gram, diag)
    high = high_ref[0] != 0
    keep_ref[...] = jnp.where(high, back, front)
    send_ref[...] = jnp.where(high, front, back)


def apply_blocks(index, high, coeff, pieces, own, base):
    slots, frames = index.shape
    vectors = own.shape[1] // 6
    vmem = pl.BlockSpec(memory_space=pltpu.VMEM)
    return pl.pallas_call(
        functools.partial(apply_kernel, pieces=len(pieces), base=base),
        in_specs=[pl.BlockSpec(memory_space=pltpu.SMEM)] * 2 + [vmem] * (2 + len(pieces)),
        out_specs=(vmem, vmem, vmem),
        out_shape=(
            pltpu.VMEM((frames * 6, vectors), f32),
            pltpu.VMEM((vectors, vectors), f32),
            pltpu.VMEM((vectors, vectors), f32),
        ),
        scratch_shapes=[
            pltpu.VMEM(((base + frames) * (own.shape[1] // 128 + 1) + 16, 128), f32),
            pltpu.VMEM((2, frames * 9 + 16, 128), f32),
        ],
        cost_estimate=pl.CostEstimate(flops=10**9, bytes_accessed=8 * 10**6, transcendentals=0),
        compiler_params=pltpu.CompilerParams(vmem_limit_bytes=24 << 20),
        name="apply_blocks",
    )(index, high, near_core(coeff), *map(near_core, pieces), own)


panel = 64


def factor_panels(blocks):
    groups = panel // 8
    sub = lax.broadcasted_iota(jnp.int32, (8, 128), 0)
    every = range(len(blocks))
    rows = [[block[g * 8 : (g + 1) * 8] for g in range(groups)] for block in blocks]

    def spread_row(x, k):
        return jnp.broadcast_to(x[k : k + 1, :], (8, 128))

    for g in range(groups):
        wide = [
            [
                [jnp.broadcast_to(rows[b][r][:, g * 8 + k : g * 8 + k + 1], (8, 128)) for k in range(8)]
                for r in range(g, groups)
            ]
            for b in every
        ]
        top = [rows[b][g] for b in every]
        full = list(top)
        scale = [jnp.zeros((8, 128), f32) for b in every]
        square = [jnp.zeros((8, 128), f32) for b in every]
        for k in range(8):
            for b in every:
                lead = wide[b][0]
                root = lax.rsqrt(spread_row(lead[k], k))
                inv = root * root
                scale[b] = jnp.where(sub == k, root, scale[b])
                square[b] = jnp.where(sub == k, inv, square[b])
                factor = jnp.where(sub != k, lead[k] * inv, 0.0)
                below = jnp.where(sub > k, factor, 0.0)
                for m in range(k + 1, 8):
                    lead[m] = lead[m] - factor * spread_row(lead[m], k)
                top[b] = top[b] - below * spread_row(top[b], k)
                full[b] = full[b] - factor * spread_row(full[b], k)
        for b in every:
            gain = full[b] * square[b]
            gain = [spread_row(gain, k) for k in range(8)]
            for r in range(g + 1, groups):
                row = rows[b][r]
                cols = wide[b][r - g]
                for k in range(8):
                    row = row - cols[k] * gain[k]
                rows[b][r] = row
        for b in every:
            rows[b][g] = top[b] * scale[b]
    return [jnp.concatenate(rows[b], axis=0) for b in every]


def solve_kernel(high_ref, mine_ref, got_ref, image_ref, next_ref, ritz_ref, image_scr, basis_scr, *, total_rows):
    size = mine_ref.shape[1]
    frames = next_ref.shape[0]
    rows = lax.broadcasted_iota(jnp.int32, (size, size), 0)
    cols = lax.broadcasted_iota(jnp.int32, (size, size), 1)
    high = high_ref[0] != 0
    mine = mine_ref[...] * (1.0 / total_rows)
    got = got_ref[...] * (1.0 / total_rows)
    mixed = jnp.where(high, got, mine)
    other = jnp.where(high, mine, got)
    turned = mixed.T
    image_gram = jnp.where(rows >= cols, mixed, turned)
    basis_gram = jnp.where(rows >= cols, other, other.T)
    last = size - 1
    diag = pltpu.roll(jnp.where(cols == rows + 1, other, 0.0), size - 1, 1)
    corner = jnp.sum(jnp.where((rows == 0) & (cols == last), other, 0.0), axis=0, keepdims=True)
    diag = diag + jnp.where(rows == last, corner, 0.0)
    cross = jnp.where(rows < cols, mixed, jnp.where(rows > cols, turned, diag)) * 0.5
    eye = jnp.where(rows == cols, 1.0, 0.0)
    scratch = (image_scr, basis_scr)
    image_scr[:, 0:size] = image_gram
    basis_scr[:, 0:size] = basis_gram
    image_scr[:, size:] = eye
    basis_scr[:, size:] = eye
    small = jnp.where(
        lax.broadcasted_iota(jnp.int32, (panel, panel), 0)
        == lax.broadcasted_iota(jnp.int32, (panel, panel), 1),
        1.0,
        0.0,
    )
    lane_ids = lax.broadcasted_iota(jnp.int32, (panel, size), 1)

    def one_panel(p, carry):
        at = pl.multiple_of(p * panel, panel)
        strips = [ref[pl.ds(at, panel), :] for ref in scratch]
        fronts = [pltpu.roll(x[:, 0:size], size - at, 1)[:, 0:panel] for x in strips]
        solved = factor_panels([jnp.concatenate([x, small], axis=1) for x in fronts])
        done = [
            jnp.dot(inv[:, panel:], x, precision=exact, preferred_element_type=f32)
            for inv, x in zip(solved, strips)
        ]
        for ref, x in zip(scratch, done):
            left = jnp.where(lane_ids >= at + panel, x[:, 0:size], 0.0)
            ref[...] = ref[...] - lax.dot_general(
                left, x, (((0,), (0,)), ((), ())), precision=exact, preferred_element_type=f32
            )
            ref[pl.ds(at, panel), :] = x
        return carry

    lax.fori_loop(0, size // panel, one_panel, 0)
    image_inv = image_scr[:, size:]
    basis_inv = basis_scr[:, size:]
    turn = (((1,), (1,)), ((), ()))
    res = lax.dot_general(image_ref[...], image_inv, turn, precision=exact, preferred_element_type=f32)
    for j in range(6):
        next_ref[:, j * size : (j + 1) * size] = res[j * frames : (j + 1) * frames]
    half = jnp.dot(basis_inv, cross, precision=exact, preferred_element_type=f32)
    ritz_ref[...] = lax.dot_general(half, basis_inv, turn, precision=exact, preferred_element_type=f32)


def solve(high, mine, got, image, total_rows):
    size = image.shape[1]
    frames = image.shape[0] // 6
    vmem = pl.BlockSpec(memory_space=pltpu.VMEM)
    return pl.pallas_call(
        functools.partial(solve_kernel, total_rows=float(total_rows)),
        in_specs=[pl.BlockSpec(memory_space=pltpu.SMEM), vmem, vmem, vmem],
        out_specs=(vmem, vmem),
        out_shape=(
            jax.ShapeDtypeStruct((frames, 6 * size), f32),
            jax.ShapeDtypeStruct((size, size), f32),
        ),
        scratch_shapes=[
            pltpu.VMEM((size, 2 * size), f32),
            pltpu.VMEM((size, 2 * size), f32),
        ],
        cost_estimate=pl.CostEstimate(flops=10**9, bytes_accessed=3 * 10**6, transcendentals=0),
        compiler_params=pltpu.CompilerParams(vmem_limit_bytes=20 << 20),
        name="solve",
    )(high, near_core(mine), near_core(got), near_core(image))


def spread(stack, axis):
    count = lax.axis_size(axis)
    if count == 1:
        return [stack]
    up = [(i, i + 1) for i in range(count - 1)]
    down = [(i + 1, i) for i in range(count - 1)]
    if count == 2:
        return [stack, lax.ppermute(stack, axis, up + down)]
    return [stack, lax.ppermute(stack, axis, up), lax.ppermute(stack, axis, down)]


def place_of(offset, axis):
    count = lax.axis_size(axis)
    if count <= 2:
        return jnp.where(offset == 1, 0, 1), count
    return jnp.where(offset == 1, 0, jnp.where(offset == 0, 1, 2)), 3


def sum_all(values, axes, done, halvings):
    steps = []
    for axis in axes:
        bit = 1
        while bit < lax.axis_size(axis):
            if (axis, bit) != done:
                steps.append((axis, bit))
            bit *= 2
    trail = []
    for n, (axis, bit) in enumerate(steps):
        pairs = [(i, i ^ bit) for i in range(lax.axis_size(axis))]
        if n >= halvings:
            values = values + lax.ppermute(values, axis, pairs)
            continue
        high = (lax.axis_index(axis) & bit) != 0
        half = values.shape[0] // 2
        front, back = values[:half], values[half:]
        got = lax.ppermute(jnp.where(high, front, back), axis, pairs)
        values = jnp.where(high, back, front) + got
        trail.append((axis, high, pairs))
    for axis, high, pairs in reversed(trail):
        got = lax.ppermute(values, axis, pairs)
        values = jnp.where(
            high, jnp.concatenate([got, values]), jnp.concatenate([values, got])
        )
    return values


def per_device(coordinates, neighbours, pair_index, pair_live, basis):
    frames, columns = basis.shape[3:]
    rim = frames // 4
    atoms = coordinates.shape[4]
    slots = neighbours.shape[3]
    count = pair_index.shape[4]
    axes = ("gx", "gy", "gz")
    total_rows = 6 * frames
    for a in axes:
        total_rows *= lax.axis_size(a)
    own_coords = coordinates[0, 0, 0]
    own_basis = basis[0, 0, 0]
    lists = neighbours[0, 0, 0]

    spots = own_coords.reshape(3 * atoms, frames)[:, :rim].T
    high = lax.reduce_precision(spots, 8, 7)
    middle = lax.reduce_precision(spots - high, 8, 7)
    width = 9 * atoms
    row = jnp.concatenate(
        [
            own_basis[:rim],
            high.astype(bf16),
            middle.astype(bf16),
            (spots - high - middle).astype(bf16),
            jnp.zeros((rim, round_up(width, 128) - width), bf16),
        ],
        axis=1,
    )
    ghost = 27 * rim
    domain = lists // rim
    px, nx = place_of(domain // 9, "gx")
    py, ny = place_of(domain // 3 % 3, "gy")
    pz, nz = place_of(domain % 3, "gz")
    base = round_up(nx * ny * nz * rim, 128)
    index = jnp.where(
        lists < ghost,
        ((py * nz + pz) * nx + px) * rim + lists % rim,
        lists - ghost + base,
    )

    chunk = 1920
    steps = count // chunk
    cut = [0, steps // 2 - 1, steps]
    table = jnp.concatenate(
        [pair_index[0, 0, 0], pair_live[0, 0], jnp.zeros((3, count), jnp.int32)], axis=0
    )
    part = jnp.concatenate(spread(row[None], "gx"), axis=0)
    table, part = lax.optimization_barrier((table, part))
    counts = count_pairs([], table, frames, slots, atoms, cut[0], cut[1] - cut[0], chunk)
    part = jnp.concatenate(spread(part, "gz"), axis=0)
    counts, part = lax.optimization_barrier((counts, part))
    near = spread(part, "gy")
    counts = count_pairs([counts], table, frames, slots, atoms, cut[1], cut[2] - cut[1], chunk)
    coeff = make_blocks(counts, near, own_coords, index, base, columns)
    axis = "gy"
    pairs = [(i, i ^ 1) for i in range(lax.axis_size(axis))]
    side = lax.axis_index(axis) % 2
    high = side[None]
    image, keep, send = apply_blocks(index, high, coeff, near, own_basis, base)
    mine = keep + lax.ppermute(send, axis, pairs)
    mine = sum_all(mine, ("gy", "gz", "gx"), (axis, 1), 1)
    got = lax.ppermute(mine, axis, pairs)
    next_rows, ritz = solve(high, mine, got, image, total_rows)
    return next_rows[None, None, None], ritz


def solution(mesh):
    placed = (
        P("gx", "gy", "gz", None, None, None),
        P("gx", "gy", "gz", None, None),
        P("gx", "gy", "gz", None, None),
        P("gx", "gy", "gz", None),
        P("gx", "gy", "gz", None, None),
    )
    return jax.shard_map(
        per_device,
        mesh=mesh,
        in_specs=placed,
        out_specs=(P("gx", "gy", "gz", None, None), P()),
        check_vma=False,
    )
```

```python
import functools

import jax
import jax.numpy as jnp
from jax import lax
from jax.experimental import pallas as pl
from jax.experimental.pallas import tpu as pltpu
from jax.sharding import PartitionSpec as P

stiffness = 0.01
radix = 4096.0
exact = lax.Precision.HIGHEST
f32 = jnp.float32
bf16 = jnp.bfloat16


def near_core(x):
    return pltpu.with_memory_space_constraint(x, pltpu.VMEM)


def round_up(value, step):
    return (value + step - 1) // step * step


def count_kernel(*refs, frames, half, first, steps, chunk):
    index_ref, *before, out_ref, done_ref = refs
    done_ref[...] = jnp.zeros_like(done_ref)
    rows, lanes = out_ref.shape[1:]
    row_ids = lax.broadcasted_iota(jnp.int32, (rows, chunk), 0).astype(jnp.int16)
    lane_ids = lax.broadcasted_iota(jnp.int32, (lanes, chunk), 0).astype(jnp.int16)
    zero = jnp.zeros((), bf16)
    out_ref[...] = before[0][...] if before else jnp.zeros_like(out_ref)

    def one_chunk(i, carry):
        at = pl.ds(pl.multiple_of((first + i) * chunk, 128), chunk)
        block = index_ref[:, at]
        frame, slot, atom_a, atom_b, live = [block[k : k + 1] for k in range(5)]
        high = atom_b >= half
        row = (slot - 1) * (half * half) + jnp.where(high, atom_b - half, atom_b) * half
        high_a = atom_a >= half
        row = row + jnp.where(high_a, atom_a - half, atom_a)
        lane = jnp.where(high_a, frames, 0) + frame
        value = jnp.where(high, radix, 1.0) * live.astype(f32)
        left = jnp.where(row_ids == row.astype(jnp.int16), value.astype(bf16), zero)
        right = jnp.where(lane_ids == lane.astype(jnp.int16), jnp.ones((), bf16), zero)
        both = lax.dot_general(
            left, right, (((1,), (1,)), ((), ())), preferred_element_type=f32
        )
        upper = jnp.floor(both * (1.0 / radix))
        out_ref[0] += both - upper * radix
        out_ref[1] += upper
        return carry

    lax.fori_loop(0, steps, one_chunk, 0)


def count_pairs(before, table, frames, slots, atoms, first, steps, chunk):
    half = atoms // 2
    rows = (slots - 1) * half * half
    vmem = pl.BlockSpec(memory_space=pltpu.VMEM)
    return pl.pallas_call(
        functools.partial(
            count_kernel, frames=frames, half=half, first=first, steps=steps, chunk=chunk
        ),
        in_specs=[vmem] * (1 + len(before)),
        out_specs=(vmem, vmem),
        out_shape=(pltpu.VMEM((2, rows, 2 * frames), f32), jax.ShapeDtypeStruct((8, 128), f32)),
        cost_estimate=pl.CostEstimate(
            flops=2 * rows * 2 * frames * chunk * steps,
            bytes_accessed=rows * frames * 16,
            transcendentals=0,
        ),
        compiler_params=pltpu.CompilerParams(vmem_limit_bytes=24 << 20),
        name="count_pairs",
    )(near_core(table), *map(near_core, before))


upper_pairs = [(i, j) for i in range(6) for j in range(i, 6)]
pair_slot = {}
for _n, (_i, _j) in enumerate(upper_pairs):
    pair_slot[(_i, _j)] = _n
    pair_slot[(_j, _i)] = _n


def split3(x):
    hi = x.astype(bf16)
    rest = x - hi.astype(f32)
    mid = rest.astype(bf16)
    low = (rest - mid.astype(f32)).astype(bf16)
    return hi, mid, low


def block_kernel(*refs, pieces, base, columns):
    count_ref = refs[0]
    piece_refs = refs[1 : 1 + pieces]
    own_ref, index_ref, out_ref, near_scr, sum_scr, arm_scr, blk_scr = refs[1 + pieces :]
    atoms, frames = own_ref.shape[1:]
    slots = index_ref.shape[0]
    half = atoms // 2
    width = 3 * atoms
    near_scr[...] = jnp.zeros_like(near_scr)
    start = 0
    for piece in piece_refs:
        for k in range(piece.shape[0]):
            near_scr[start : start + piece.shape[1], :] = piece[k, :, columns:].astype(f32)
            start += piece.shape[1]
    near = near_scr[...].T[0 : 3 * width].astype(bf16)
    near = [near[k * width : (k + 1) * width] for k in range(3)]
    own = own_ref[...].reshape(width, frames)
    parts = [jnp.concatenate([n, o], axis=1) for n, o in zip(near, split3(own))]
    left = jnp.concatenate(parts, axis=0)
    rows = base + frames
    row_ids = lax.broadcasted_iota(jnp.int32, (rows, frames), 0)
    pos = [own_ref[c] for c in range(3)]
    centre = [jnp.mean(p, axis=0, keepdims=True) for p in pos]
    pos_t = [[p[h * half : (h + 1) * half] for h in range(2)] for p in pos]
    rho_t = [[p - c for p in pt] for pt, c in zip(pos_t, centre)]
    sum_scr[...] = jnp.zeros_like(sum_scr)
    arm_scr[...] = jnp.zeros_like(arm_scr)

    def one_slot(s, carry):
        pick = index_ref[pl.ds(s, 1), :]
        hot = jnp.where(row_ids == pick, 1.0, 0.0).astype(bf16)
        got = jnp.dot(left, hot, preferred_element_type=f32)
        far = got[0:width] + got[width : 2 * width] + got[2 * width : 3 * width]
        far = [far[c * atoms : (c + 1) * atoms] for c in range(3)]
        for c in range(3):
            arm_scr[c, pl.ds(s, 1), :] = jnp.mean(far[c], axis=0, keepdims=True) - centre[c]
        moments = [[None] * 6 for _ in range(2)]
        for b in range(atoms):
            at = pl.multiple_of((s - 1) * (half * half) + (b % half) * half, half)
            q = [jnp.broadcast_to(far[c][b : b + 1, :], (half, frames)) for c in range(3)]
            for h in range(2):
                lanes = slice(h * frames, (h + 1) * frames)
                n = count_ref[b // half, pl.ds(at, half), lanes]
                d = [pos_t[c][h] - q[c] for c in range(3)]
                w = n / jnp.maximum(d[0] * d[0] + d[1] * d[1] + d[2] * d[2], 1.0)
                wd = [w * d[c] for c in range(3)]
                terms = [wd[0] * d[0], wd[0] * d[1], wd[0] * d[2], wd[1] * d[1], wd[1] * d[2], wd[2] * d[2]]
                m = moments[h]
                moments[h] = terms if m[0] is None else [x + y for x, y in zip(m, terms)]
        total = [None] * 21
        for h in range(2):
            m = moments[h]
            r = [rho_t[c][h] for c in range(3)]
            dd = [[m[0], m[1], m[2]], [m[1], m[3], m[4]], [m[2], m[4], m[5]]]
            dt = [
                [
                    r[1] * dd[i][2] - r[2] * dd[i][1],
                    r[2] * dd[i][0] - r[0] * dd[i][2],
                    r[0] * dd[i][1] - r[1] * dd[i][0],
                ]
                for i in range(3)
            ]
            tt = {}
            for j in range(3):
                col = [dt[0][j], dt[1][j], dt[2][j]]
                tt[(0, j)] = r[1] * col[2] - r[2] * col[1]
                tt[(1, j)] = r[2] * col[0] - r[0] * col[2]
                tt[(2, j)] = r[0] * col[1] - r[1] * col[0]
            for n, (i, j) in enumerate(upper_pairs):
                if j < 3:
                    x = dd[i][j]
                elif i < 3:
                    x = dt[i][j - 3]
                else:
                    x = tt[(i - 3, j - 3)]
                total[n] = x if total[n] is None else total[n] + x
        for n in range(21):
            sum_scr[n, pl.ds(s, 1), :] = jnp.sum(total[n], axis=0, keepdims=True) * stiffness
        return carry

    lax.fori_loop(1, slots, one_slot, 0)
    first = lax.broadcasted_iota(jnp.int32, (slots, frames), 0) == 0
    arm = [arm_scr[c] for c in range(3)]
    sums = [sum_scr[n] for n in range(21)]
    selfs = [jnp.sum(x, axis=0, keepdims=True) for x in sums]
    blk_scr[...] = jnp.zeros_like(blk_scr)
    out_ref[...] = jnp.zeros_like(out_ref)
    for j in range(6):
        for i in range(6):
            x = sums[pair_slot[(j, i)]]
            if i >= 3:
                p, q = (i - 2) % 3, (i - 1) % 3
                x = x - (arm[p] * sums[pair_slot[(j, q)]] - arm[q] * sums[pair_slot[(j, p)]])
            x = jnp.where(first, selfs[pair_slot[(j, i)]], -x)
            for h in range(2):
                blk_scr[j, pl.ds(2 * i + h, slots, stride=17), :] = x
        turned = jnp.concatenate([blk_scr[j, s * 17 : s * 17 + 16, :] for s in range(slots)], axis=0).T
        for h in range(turned.shape[1] // 128):
            out_ref[h, pl.ds(j, frames, stride=9), :] = turned[:, h * 128 : (h + 1) * 128]


def make_blocks(counts, pieces, own, index, base, columns):
    slots, frames = index.shape
    vmem = pl.BlockSpec(memory_space=pltpu.VMEM)
    return pl.pallas_call(
        functools.partial(block_kernel, pieces=len(pieces), base=base, columns=columns),
        in_specs=[vmem] * (3 + len(pieces)),
        out_specs=vmem,
        out_shape=pltpu.VMEM((slots // 8, frames * 9 + 16, 128), f32),
        scratch_shapes=[
            pltpu.VMEM((base, pieces[0].shape[2] - columns), f32),
            pltpu.VMEM((21, slots, frames), f32),
            pltpu.VMEM((3, slots, frames), f32),
            pltpu.VMEM((6, slots * 17 + 17, frames), f32),
        ],
        cost_estimate=pl.CostEstimate(flops=10**9, bytes_accessed=8 * 10**6, transcendentals=0),
        compiler_params=pltpu.CompilerParams(vmem_limit_bytes=20 << 20),
        name="make_blocks",
    )(near_core(counts), *map(near_core, pieces), near_core(own), near_core(index))


def apply_kernel(*refs, pieces, base):
    index_ref, high_ref, coeff_ref = refs[:3]
    piece_refs = refs[3 : 3 + pieces]
    own_ref, image_ref, keep_ref, send_ref, tab_scr, image_scr = refs[3 + pieces :]
    frames = own_ref.shape[0]
    slots = index_ref.shape[0]
    vectors = own_ref.shape[1] // 6
    tiles = own_ref.shape[1] // 128
    pitch = tiles + 1
    rim = piece_refs[0].shape[1]
    start = 0
    for piece in piece_refs:

        def fill(k, carry, piece=piece, start=start):
            at = (start + k) * (rim * pitch)
            for t in range(tiles):
                part = piece[k, :, t * 128 : (t + 1) * 128].astype(f32)
                tab_scr[pl.ds(at + t, rim, stride=pitch), :] = part
            tab_scr[pl.ds(at + tiles, rim, stride=pitch), :] = jnp.zeros((rim, 128), f32)
            return carry

        lax.fori_loop(0, piece.shape[0], fill, 0)
        start += piece.shape[0]
    for t in range(tiles):
        part = own_ref[:, t * 128 : (t + 1) * 128].astype(f32)
        tab_scr[pl.ds(base * pitch + t, frames, stride=pitch), :] = part
    tab_scr[pl.ds(base * pitch + tiles, frames, stride=pitch), :] = jnp.zeros((frames, 128), f32)
    tab_scr[(base + frames) * pitch :, :] = jnp.zeros((16, 128), f32)
    odd = lax.broadcasted_iota(jnp.int32, (8, slots * 16), 1) % 2 == 1

    def one_frame(f, carry):
        got = []
        for s in range(slots):
            got.append(tab_scr[pl.ds(index_ref[s, f] * pitch, 16), :].astype(bf16))
        right = jnp.concatenate(got, axis=0)
        at = f * 9
        coeff = jnp.concatenate([coeff_ref[h, pl.ds(at, 8), :] for h in range(slots // 8)], axis=1)
        wide = jnp.concatenate([jnp.where(odd, 0.0, coeff), jnp.where(odd, coeff, 0.0)], axis=0)
        high = wide.astype(bf16)
        low = (wide - high.astype(f32)).astype(bf16)
        res = jnp.dot(jnp.concatenate([high, low], axis=0), right, preferred_element_type=f32)
        res = res[0:16] + res[16:32]
        image_scr[0, pl.ds(at, 8), :] = res[0:8]
        image_scr[1, pl.ds(at, 8), :] = res[8:16]
        return carry

    lax.fori_loop(0, frames, one_frame, 0, unroll=32)
    dims = (((0,), (0,)), ((), ()))
    basis_gram = jnp.zeros((vectors, vectors), f32)
    cross = jnp.zeros((vectors, vectors), f32)
    image_gram = jnp.zeros((vectors, vectors), f32)
    for j in range(6):
        x = own_ref[:, j * vectors : (j + 1) * vectors]
        y = jnp.concatenate([image_scr[h, pl.ds(j, frames, stride=9), :] for h in range(2)], axis=1)
        image_ref[j * frames : (j + 1) * frames, :] = y
        y = y.astype(bf16)
        basis_gram = basis_gram + lax.dot_general(x, x, dims, preferred_element_type=f32)
        cross = cross + lax.dot_general(x, y, dims, preferred_element_type=f32)
        image_gram = image_gram + lax.dot_general(y, y, dims, preferred_element_type=f32)
    cross = cross + cross.T
    rows = lax.broadcasted_iota(jnp.int32, cross.shape, 0)
    cols = lax.broadcasted_iota(jnp.int32, cross.shape, 1)
    part = vectors // 2
    diag = jnp.sum(jnp.where(rows == cols, cross, 0.0), axis=0, keepdims=True)
    low = basis_gram[part:, part:].T
    edge = rows[0:part, 0:part] == cols[0:part, 0:part]
    low_diag = jnp.sum(jnp.where(edge, low, 0.0), axis=0, keepdims=True)
    square = jnp.where(rows[0:part, 0:part] >= cols[0:part, 0:part], basis_gram[0:part, 0:part], low)
    mixed = jnp.where(rows >= cols, image_gram, cross)
    cut = keep_ref.shape[0]
    front = mixed[0:cut]
    back = jnp.concatenate(
        [
            mixed[cut:],
            jnp.concatenate([square, basis_gram[part:, 0:part]], axis=1),
            jnp.broadcast_to(diag, (8, vectors)),
            jnp.broadcast_to(jnp.concatenate([low_diag, low_diag], axis=1), (8, vectors)),
            jnp.zeros((2 * cut - 3 * part - 16, vectors), f32),
        ],
        axis=0,
    )
    high = high_ref[0] != 0
    keep_ref[...] = jnp.where(high, back, front)
    send_ref[...] = jnp.where(high, front, back)


def apply_blocks(index, high, coeff, pieces, own, base):
    slots, frames = index.shape
    vectors = own.shape[1] // 6
    cut = round_up(3 * vectors // 2 + 16, 32) // 2
    vmem = pl.BlockSpec(memory_space=pltpu.VMEM)
    return pl.pallas_call(
        functools.partial(apply_kernel, pieces=len(pieces), base=base),
        in_specs=[pl.BlockSpec(memory_space=pltpu.SMEM)] * 2 + [vmem] * (2 + len(pieces)),
        out_specs=(vmem, vmem, vmem),
        out_shape=(
            pltpu.VMEM((frames * 6, vectors), f32),
            pltpu.VMEM((cut, vectors), f32),
            pltpu.VMEM((cut, vectors), f32),
        ),
        scratch_shapes=[
            pltpu.VMEM(((base + frames) * (own.shape[1] // 128 + 1) + 16, 128), f32),
            pltpu.VMEM((2, frames * 9 + 16, 128), f32),
        ],
        cost_estimate=pl.CostEstimate(flops=10**9, bytes_accessed=8 * 10**6, transcendentals=0),
        compiler_params=pltpu.CompilerParams(vmem_limit_bytes=24 << 20),
        name="apply_blocks",
    )(index, high, near_core(coeff), *map(near_core, pieces), near_core(own))


panel = 128


def factor_panels(blocks):
    groups = panel // 8
    sub = lax.broadcasted_iota(jnp.int32, (8, 128), 0)
    every = range(len(blocks))
    tiles = range(2)
    rows = [[[t[g * 8 : (g + 1) * 8] for t in block] for g in range(groups)] for block in blocks]

    def spread_row(x, k):
        return jnp.broadcast_to(x[k : k + 1, :], (8, 128))

    def columns(b, r, g):
        return [jnp.broadcast_to(rows[b][r][0][:, g * 8 + k : g * 8 + k + 1], (8, 128)) for k in range(8)]

    def update(b, r, cols, gain):
        for t in tiles:
            for k in range(8):
                rows[b][r][t] = rows[b][r][t] - cols[k] * gain[b][t][k]

    for g in range(groups):
        leads = [columns(b, g, g) for b in every]
        top = [list(rows[b][g]) for b in every]
        full = [list(rows[b][g]) for b in every]
        scale = [jnp.zeros((8, 128), f32) for b in every]
        square = [jnp.zeros((8, 128), f32) for b in every]
        for k in range(8):
            for b in every:
                lead = leads[b]
                root = lax.rsqrt(spread_row(lead[k], k))
                inv = root * root
                scale[b] = jnp.where(sub == k, root, scale[b])
                square[b] = jnp.where(sub == k, inv, square[b])
                factor = jnp.where(sub != k, lead[k] * inv, 0.0)
                below = jnp.where(sub > k, factor, 0.0)
                for m in range(k + 1, 8):
                    lead[m] = lead[m] - factor * spread_row(lead[m], k)
                for t in tiles:
                    top[b][t] = top[b][t] - below * spread_row(top[b][t], k)
                    full[b][t] = full[b][t] - factor * spread_row(full[b][t], k)
        gain = [[x * square[b] for x in full[b]] for b in every]
        gain = [[[spread_row(x, k) for k in range(8)] for x in gain[b]] for b in every]
        for b in every:
            for r in range(g + 1, groups):
                update(b, r, columns(b, r, g), gain)
        for b in every:
            rows[b][g] = [x * scale[b] for x in top[b]]
    return [jnp.concatenate([rows[b][g][1] for g in range(groups)], axis=0) for b in every]


def solve_kernel(high_ref, mine_ref, got_ref, image_ref, next_ref, ritz_ref, image_scr, basis_scr, *, total_rows):
    size = mine_ref.shape[1]
    frames = next_ref.shape[0]
    rows = lax.broadcasted_iota(jnp.int32, (size, size), 0)
    cols = lax.broadcasted_iota(jnp.int32, (size, size), 1)
    high = high_ref[0] != 0
    mine = mine_ref[...] * (1.0 / total_rows)
    got = got_ref[...] * (1.0 / total_rows)
    cut = mine.shape[0]
    part = size // 2
    front = jnp.where(high, got, mine)
    back = jnp.where(high, mine, got)
    mixed = jnp.concatenate([front, back[0 : size - cut]], axis=0)
    at = size - cut
    square = back[at : at + part, 0:part]
    side = back[at : at + part, part:]
    at += part
    diag = back[at : at + 1]
    low_diag = back[at + 8 : at + 9, 0:part]
    turned = mixed.T
    square_t = square.T
    image_gram = jnp.where(rows >= cols, mixed, turned)
    r, c = rows[0:part, 0:part], cols[0:part, 0:part]
    first = jnp.where(r >= c, square, square_t)
    second = jnp.where(r < c, square, jnp.where(r > c, square_t, low_diag))
    basis_gram = jnp.concatenate(
        [jnp.concatenate([first, side.T], axis=1), jnp.concatenate([side, second], axis=1)], axis=0
    )
    cross = jnp.where(rows < cols, mixed, jnp.where(rows > cols, turned, diag)) * 0.5
    eye = jnp.where(rows == cols, 1.0, 0.0)
    scratch = (image_scr, basis_scr)
    image_scr[:, 0:size] = image_gram
    basis_scr[:, 0:size] = basis_gram
    image_scr[:, size:] = eye
    basis_scr[:, size:] = eye
    small = jnp.where(
        lax.broadcasted_iota(jnp.int32, (panel, panel), 0)
        == lax.broadcasted_iota(jnp.int32, (panel, panel), 1),
        1.0,
        0.0,
    )

    for at in range(0, size, panel):
        strips = [ref[at : at + panel, :] for ref in scratch]
        solved = factor_panels([(x[:, at : at + panel], small) for x in strips])
        done = [
            jnp.dot(inv, x, precision=exact, preferred_element_type=f32)
            for inv, x in zip(solved, strips)
        ]
        for ref, x in zip(scratch, done):
            ref[at : at + panel, :] = x
            for r in range(at + panel, size, panel):
                left = x[:, r : r + panel]
                ref[r : r + panel, :] = ref[r : r + panel, :] - lax.dot_general(
                    left, x, (((0,), (0,)), ((), ())), precision=exact, preferred_element_type=f32
                )
    image_inv = image_scr[:, size:]
    basis_inv = basis_scr[:, size:]
    turn = (((1,), (1,)), ((), ()))
    res = lax.dot_general(image_ref[...], image_inv, turn, precision=exact, preferred_element_type=f32)
    for j in range(6):
        next_ref[:, j * size : (j + 1) * size] = res[j * frames : (j + 1) * frames]
    half = jnp.dot(basis_inv, cross, precision=exact, preferred_element_type=f32)
    ritz_ref[...] = lax.dot_general(half, basis_inv, turn, precision=exact, preferred_element_type=f32)


def solve(high, mine, got, image, total_rows):
    size = image.shape[1]
    frames = image.shape[0] // 6
    vmem = pl.BlockSpec(memory_space=pltpu.VMEM)
    return pl.pallas_call(
        functools.partial(solve_kernel, total_rows=float(total_rows)),
        in_specs=[pl.BlockSpec(memory_space=pltpu.SMEM), vmem, vmem, vmem],
        out_specs=(vmem, vmem),
        out_shape=(
            jax.ShapeDtypeStruct((frames, 6 * size), f32),
            jax.ShapeDtypeStruct((size, size), f32),
        ),
        scratch_shapes=[
            pltpu.VMEM((size, 2 * size), f32),
            pltpu.VMEM((size, 2 * size), f32),
        ],
        cost_estimate=pl.CostEstimate(flops=10**9, bytes_accessed=3 * 10**6, transcendentals=0),
        compiler_params=pltpu.CompilerParams(vmem_limit_bytes=20 << 20),
        name="solve",
    )(high, near_core(mine), near_core(got), near_core(image))


def spread(stack, axis):
    count = lax.axis_size(axis)
    if count == 1:
        return [stack]
    up = [(i, i + 1) for i in range(count - 1)]
    down = [(i + 1, i) for i in range(count - 1)]
    if count == 2:
        return [stack, lax.ppermute(stack, axis, up + down)]
    return [stack, lax.ppermute(stack, axis, up), lax.ppermute(stack, axis, down)]


def place_of(offset, axis):
    count = lax.axis_size(axis)
    if count <= 2:
        return jnp.where(offset == 1, 0, 1), count
    return jnp.where(offset == 1, 0, jnp.where(offset == 0, 1, 2)), 3


def sum_all(values, axes, done, halvings):
    steps = []
    for axis in axes:
        bit = 1
        while bit < lax.axis_size(axis):
            if (axis, bit) != done:
                steps.append((axis, bit))
            bit *= 2
    trail = []
    for n, (axis, bit) in enumerate(steps):
        pairs = [(i, i ^ bit) for i in range(lax.axis_size(axis))]
        if n >= halvings:
            values = values + lax.ppermute(values, axis, pairs)
            continue
        high = (lax.axis_index(axis) & bit) != 0
        half = values.shape[0] // 2
        front, back = values[:half], values[half:]
        got = lax.ppermute(jnp.where(high, front, back), axis, pairs)
        values = jnp.where(high, back, front) + got
        trail.append((axis, high, pairs))
    for axis, high, pairs in reversed(trail):
        got = lax.ppermute(values, axis, pairs)
        values = jnp.where(
            high, jnp.concatenate([got, values]), jnp.concatenate([values, got])
        )
    return values


def per_device(coordinates, neighbours, pair_index, pair_live, basis):
    frames, columns = basis.shape[3:]
    rim = frames // 4
    atoms = coordinates.shape[4]
    slots = neighbours.shape[3]
    count = pair_index.shape[4]
    axes = ("gx", "gy", "gz")
    total_rows = 6 * frames
    for a in axes:
        total_rows *= lax.axis_size(a)
    own_coords = coordinates[0, 0, 0]
    own_basis = basis[0, 0, 0]
    lists = neighbours[0, 0, 0]

    spots = own_coords.reshape(3 * atoms, frames)[:, :rim].T
    high = lax.reduce_precision(spots, 8, 7)
    middle = lax.reduce_precision(spots - high, 8, 7)
    width = 9 * atoms
    row = jnp.concatenate(
        [
            own_basis[:rim],
            high.astype(bf16),
            middle.astype(bf16),
            (spots - high - middle).astype(bf16),
            jnp.zeros((rim, round_up(width, 128) - width), bf16),
        ],
        axis=1,
    )
    ghost = 27 * rim
    domain = lists // rim
    px, nx = place_of(domain // 9, "gx")
    py, ny = place_of(domain // 3 % 3, "gy")
    pz, nz = place_of(domain % 3, "gz")
    base = round_up(nx * ny * nz * rim, 128)
    index = jnp.where(
        lists < ghost,
        ((py * nz + pz) * nx + px) * rim + lists % rim,
        lists - ghost + base,
    )

    chunk = 1920
    steps = count // chunk
    cut = [0, steps // 2 - 1, steps]
    table = jnp.concatenate(
        [pair_index[0, 0, 0], pair_live[0, 0], jnp.zeros((3, count), jnp.int32)], axis=0
    )
    part = jnp.concatenate(spread(row[None], "gx"), axis=0)
    table, part = lax.optimization_barrier((table, part))
    counts, done = count_pairs([], table, frames, slots, atoms, cut[0], cut[1] - cut[0], chunk)
    part = jnp.concatenate(spread(part, "gz"), axis=0)
    part = part + done[0, 0].astype(bf16)
    near = spread(part, "gy")
    counts, done = count_pairs([counts], table, frames, slots, atoms, cut[1], cut[2] - cut[1], chunk)
    coeff = make_blocks(counts, near, own_coords, index, base, columns)
    axis = "gy"
    pairs = [(i, i ^ 1) for i in range(lax.axis_size(axis))]
    side = lax.axis_index(axis) % 2
    high = side[None]
    image, keep, send = apply_blocks(index, high, coeff, near, own_basis, base)
    mine = keep + lax.ppermute(send, axis, pairs)
    mine = sum_all(mine, ("gy", "gz", "gx"), (axis, 1), 1)
    got = lax.ppermute(mine, axis, pairs)
    next_rows, ritz = solve(high, mine, got, image, total_rows)
    return next_rows[None, None, None], ritz


def solution(mesh):
    placed = (
        P("gx", "gy", "gz", None, None, None),
        P("gx", "gy", "gz", None, None),
        P("gx", "gy", "gz", None, None),
        P("gx", "gy", "gz", None),
        P("gx", "gy", "gz", None, None),
    )
    return jax.shard_map(
        per_device,
        mesh=mesh,
        in_specs=placed,
        out_specs=(P("gx", "gy", "gz", None, None), P()),
        check_vma=False,
    )
```
